8 devices in a mesh: rep: 1 (over z), dp: 8 (over x, y, core).
Axes of the slice: x: 2, y: 2, z: 1, core: 2. Of those that a mesh axis runs over, the one named last changes fastest.
Arguments:
- x: bfloat16 [8, 2048, 1024], P(('rep', 'dp'))
- dy: bfloat16 [8, 2048, 1024], P(('rep', 'dp'))
- w_gate: bfloat16 [2, 1024, 6144], P(None, 'dp')
- w_up: bfloat16 [2, 1024, 6144], P(None, 'dp')
- w_down: bfloat16 [2, 6144, 1024], P(None, 'dp')
Outputs:
- output 1: bfloat16 [8, 2048, 1024], P(('rep', 'dp'))
- output 2: bfloat16 [2, 1024, 6144], P('rep', 'dp')
- output 3: bfloat16 [2, 1024, 6144], P('rep', 'dp')
- output 4: bfloat16 [2, 6144, 1024], P('rep', 'dp')
All inputs are finite; a program needn't handle non-finite values.
Results may differ from the reference program's by a relative error of at most 0.018.
Values are sent between devices in bfloat16 or wider.
A program may use at most 2 GiB of HBM per device.

```python
import jax
import jax.numpy as jnp
from jax import lax

SEQUENCES = 8
TOKENS = 2048
D = 1024
FF = 6144
LAYERS = 2
NAMES = ("w_gate", "w_up", "w_down")
SHAPES = {"w_gate": (LAYERS, D, FF), "w_up": (LAYERS, D, FF), "w_down": (LAYERS, FF, D)}


def bump(key, n, height):
    away = (jnp.arange(n, dtype=jnp.int32) - jax.random.randint(key, (), 0, n, jnp.int32)) % n
    return jnp.where(away < n // 8, height, 1.0)


def together(key, own, strength):
    shared = jax.random.normal(key, own.shape[1:], jnp.float32)
    return (own + strength * shared) * lax.rsqrt(1 + strength * strength)


def setup_inputs(seed: int = 0, part: int = 0) -> dict:
    kx, kdy, ka, kb, kz, kf, kh, kl, *kw = jax.random.split(jax.random.key(seed), 8 + len(NAMES))
    kx, kdy, ka, kb = (jax.random.fold_in(k, part) for k in (kx, kdy, ka, kb))
    shape = (SEQUENCES, TOKENS, D)
    much_x, much_dy = jax.random.uniform(kz, (2,), jnp.float32, 0.0, 1.0)
    layers = 2.0 ** jax.random.uniform(kl, (LAYERS, 1, 1), jnp.float32, -1.0, 1.0)
    x = together(ka, jax.random.normal(kx, shape, jnp.float32), much_x) * bump(kf, D, 4.0)
    dy = together(kb, jax.random.normal(kdy, shape, jnp.float32), much_dy)
    drawn = {"x": x.astype(jnp.bfloat16), "dy": (dy * (SEQUENCES * TOKENS) ** -0.5).astype(jnp.bfloat16)}
    for key, name in zip(kw, NAMES, strict=True):
        w = jax.random.normal(key, SHAPES[name], jnp.float32) * SHAPES[name][1] ** -0.5
        drawn[name] = (w * {"w_gate": 1.0, "w_up": bump(kh, FF, 4.0), "w_down": layers}[name]).astype(jnp.bfloat16)
    return drawn


def matmul(a, w):
    return jnp.dot(a, w, preferred_element_type=jnp.float32).astype(jnp.bfloat16)


def normed(h):
    wide = h.astype(jnp.float32)
    scale = lax.rsqrt(jnp.mean(wide**2, -1, keepdims=True) + 1e-6)
    return (wide * scale).astype(jnp.bfloat16)


def layer(h, w):
    a = normed(h)
    gate = jnp.dot(a, w["w_gate"], preferred_element_type=jnp.float32)
    up = jnp.dot(a, w["w_up"], preferred_element_type=jnp.float32)
    return h + matmul((jax.nn.silu(gate) * up).astype(jnp.bfloat16), w["w_down"])


def stack(weights, h):
    return lax.scan(lambda h, w: (layer(h, w), None), h, weights)[0]


def reference(x, dy, w_gate, w_up, w_down):
    weights = dict(zip(NAMES, (w_gate, w_up, w_down), strict=True))

    def take(so_far, sequence):
        h, by_y = sequence
        _, back = jax.vjp(stack, weights, h)
        by_weights, by_h = back(by_y)
        return jax.tree.map(lambda total, term: total + term.astype(jnp.float32), so_far, by_weights), by_h

    none_yet = {name: jnp.zeros(w.shape, jnp.float32) for name, w in weights.items()}
    by_weights, by_x = lax.scan(take, none_yet, (x, dy))
    return (by_x, *(by_weights[name].astype(jnp.bfloat16) for name in NAMES))
```

```python
import jax
import jax.numpy as jnp
from jax import lax
from jax.experimental import pallas as pl
from jax.experimental.pallas import tpu as pltpu
from jax.sharding import PartitionSpec as P

F32, BF16 = jnp.float32, jnp.bfloat16
NN = (((1,), (0,)), ((), ()))
NT = (((1,), (1,)), ((), ()))
TN = (((0,), (0,)), ((), ()))
ONE = pl.Buffered(1)

NEXT = (1, 3, 0, 2)
PREV = (2, 0, 3, 1)
RIGHT = [(2 * c + k, 2 * NEXT[c] + k) for c in range(4) for k in range(2)]
LEFT = [(2 * c + k, 2 * PREV[c] + k) for c in range(4) for k in range(2)]
ACROSS = [(d, d ^ 1) for d in range(8)]
ORDER = [[2 * chip + core for core in (1 - k, k) for chip in (3 - c, PREV[c], NEXT[c], c)] for c in range(4) for k in range(2)]


def dot(a, b, dims):
    return lax.dot_general(a, b, dims, preferred_element_type=F32)


def shape(dims, dtype):
    return jax.ShapeDtypeStruct(dims, dtype)


def call(body, grid, ins, outs, flops, nbytes, name, prefetch=0, scratch=(), vmem=62 * 2**20):
    spec = pltpu.PrefetchScalarGridSpec(
        num_scalar_prefetch=prefetch, grid=grid, in_specs=ins, out_specs=[s for s, _ in outs], scratch_shapes=list(scratch)
    )
    made = pl.pallas_call(
        body,
        grid_spec=spec,
        out_shape=[o for _, o in outs],
        name=name,
        cost_estimate=pl.CostEstimate(flops=flops, bytes_accessed=nbytes, transcendentals=0),
        compiler_params=pltpu.CompilerParams(vmem_limit_bytes=vmem, dimension_semantics=("arbitrary",) * len(grid)),
    )
    return lambda *args: made(*args)[0] if len(outs) == 1 else made(*args)


def turned(order, a):
    T, D = a.shape
    b = D // 8

    def body(order_ref, a_ref, o_ref):
        o_ref[...] = a_ref[...].T

    return call(
        body, (8,), [pl.BlockSpec((T, b), lambda i, o: (0, o[i]))], [(pl.BlockSpec((b, T), lambda i, o: (i, 0)), shape((D, T), a.dtype))],
        T * D * 8, T * D * 4, "turned", prefetch=1,
    )(order, a)


def by_rows(at, d, half, got=None, bn=1024):
    T, N = d.shape
    rows = at.shape[0] // 2

    def body(a_ref, d_ref, *rest):
        t = dot(a_ref[...], d_ref[...], NN)
        if got is not None:
            t = t + rest[0][...].astype(F32)
        rest[-1][...] = t.astype(BF16)

    ins = [pl.BlockSpec((rows, T), lambda j: (half, 0), pipeline_mode=ONE), pl.BlockSpec((T, bn), lambda j: (0, j))]
    args = [at, d]
    if got is not None:
        ins.append(pl.BlockSpec((rows, bn), lambda j: (0, j)))
        args.append(got)
    return call(
        body, (N // bn,), ins, [(pl.BlockSpec((rows, bn), lambda j: (0, j)), shape((rows, N), BF16))], 2 * rows * T * N, T * N * 2, "by_rows"
    )(*args)


def by_blocks(order, p, d, got=None):
    T, D = d.shape
    n, bm = order.shape[0], p.shape[1] // 8

    def body(order_ref, p_ref, d_ref, *rest):
        t = dot(p_ref[...], d_ref[...], TN)
        if got is not None:
            t = t + rest[0][...].astype(F32)
        rest[-1][...] = t.astype(BF16)

    row = lambda i, o: (i, 0)
    ins = [pl.BlockSpec((T, bm), lambda i, o: (0, o[i])), pl.BlockSpec((T, D), lambda i, o: (0, 0), pipeline_mode=ONE)]
    args = [order, p, d]
    if got is not None:
        ins.append(pl.BlockSpec((bm, D), row))
        args.append(got)
    return call(
        body, (n,), ins, [(pl.BlockSpec((bm, D), row), shape((n * bm, D), BF16))], 2 * n * bm * T * D, T * n * bm * 2, "by_blocks", prefetch=1
    )(*args)


def right(t): return lax.ppermute(t, "dp", RIGHT)
def left(t): return lax.ppermute(t, "dp", LEFT)
def across(t): return lax.ppermute(t, "dp", ACROSS)


def gathered(w):
    return lax.all_gather(w, "dp", tiled=True)


def scattered(s):
    n = s.shape[0] // 4
    h = n // 2
    oa, ob, la, lb, ra, rb = (s[i * h:(i + 1) * h] for i in range(6))
    own = s[3 * n:]
    from_left, from_right = right(oa), left(ob)
    far_l, far_r = right(rb), left(la)
    near_l = right((ra.astype(F32) + from_left.astype(F32)).astype(BF16))
    near_r = left((lb.astype(F32) + from_right.astype(F32)).astype(BF16))
    top = own[:h].astype(F32) + near_l.astype(F32) + far_r.astype(F32)
    low = own[h:].astype(F32) + far_l.astype(F32) + near_r.astype(F32)
    return jnp.concatenate([top, low]).astype(BF16)


def normed(h):
    wide = h.astype(F32)
    scale = lax.rsqrt(jnp.mean(wide**2, -1, keepdims=True) + 1e-6)
    return (wide * scale).astype(BF16)


def solution(mesh):
    def step(x, dy, wg, wu, wd):
        order = jnp.asarray(ORDER, jnp.int32)[lax.axis_index("dp")]
        theirs, mine = order[:4], order[4:]
        h, g = x[0], dy[0]
        layers = wg.shape[0]
        saved = []
        for i in range(layers):
            gate_w, up_w, down_w = gathered(wg[i]), gathered(wu[i]), gathered(wd[i])
            a = normed(h)
            gate = dot(a, gate_w, NN)
            up = dot(a, up_w, NN)
            act = (jax.nn.silu(gate) * up).astype(BF16)
            saved.append((h, a, gate, up, act, gate_w, up_w, down_w))
            if i < layers - 1:
                h = h + dot(act, down_w, NN).astype(BF16)
        dwg, dwu, dwd = [None] * layers, [None] * layers, [None] * layers
        for i in reversed(range(layers)):
            h, a, gate, up, act, gate_w, up_w, down_w = saved[i]
            dwd[i] = scattered(by_blocks(mine, act, g, across(by_blocks(theirs, act, g))))
            at = turned(order, a)
            dp = dot(g, down_w, NT).astype(BF16).astype(F32)
            s = jax.nn.sigmoid(gate)
            du = (dp * (gate * s)).astype(BF16)
            dg = (dp * up * (s * (1 + gate * (1 - s)))).astype(BF16)
            dwg[i] = scattered(by_rows(at, dg, 1, across(by_rows(at, dg, 0))))
            dwu[i] = scattered(by_rows(at, du, 1, across(by_rows(at, du, 0))))
            da = (dot(dg, gate_w, NT).astype(BF16) + dot(du, up_w, NT).astype(BF16)).astype(F32)
            wide = h.astype(F32)
            scale = lax.rsqrt(jnp.mean(wide**2, -1, keepdims=True) + 1e-6)
            inner = jnp.mean(da * wide, -1, keepdims=True)
            g = g + (da * scale - wide * (scale * scale * scale * inner)).astype(BF16)
        return g[None], jnp.stack(dwg), jnp.stack(dwu), jnp.stack(dwd)

    data, rows = P(("rep", "dp"), None, None), P(None, "dp", None)
    out = P("rep", "dp", None)
    return jax.shard_map(step, mesh=mesh, in_specs=(data, data, rows, rows, rows), out_specs=(data, out, out, out), check_vma=False)
```

```python
import functools

import jax
import jax.numpy as jnp
from jax import lax
from jax.experimental import pallas as pl
from jax.experimental.pallas import tpu as pltpu
from jax.sharding import PartitionSpec as P


F32, BF16 = jnp.float32, jnp.bfloat16
NN = (((1,), (0,)), ((), ()))
NT = (((1,), (1,)), ((), ()))
TN = (((0,), (0,)), ((), ()))
ONE = pl.Buffered(1)

NEXT = (1, 3, 0, 2)
PREV = (2, 0, 3, 1)
RIGHT = [(2 * c + k, 2 * NEXT[c] + k) for c in range(4) for k in range(2)]
LEFT = [(2 * c + k, 2 * PREV[c] + k) for c in range(4) for k in range(2)]
ACROSS = [(d, d ^ 1) for d in range(8)]
ORDER = [[2 * chip + core for core in (1 - k, k) for chip in (3 - c, PREV[c], NEXT[c], c)] for c in range(4) for k in range(2)]


def dot(a, b, dims):
    return lax.dot_general(a, b, dims, preferred_element_type=F32)


def shape(dims, dtype):
    return jax.ShapeDtypeStruct(dims, dtype)


def place():
    me = lax.axis_index("dp")
    x, y, k = me // 4, (me // 2) % 2, me % 2
    return me, (2 * y + 1 - x) * 2 + k, (2 * (1 - y) + x) * 2 + k, me + 1 - 2 * k


def gather_copies(own, whole, send, recv):
    me, nxt, prv, other = place()
    n = whole.shape[0] // 8
    half = n // 2
    rows = lambda d, start=0, size=n: whole.at[pl.ds(pl.multiple_of(d * n + start, 8), size)]
    opp = 6 - me + 2 * (me % 2)

    def copy(i, src, dst, to):
        return pltpu.make_async_remote_copy(
            src_ref=src, dst_ref=dst, send_sem=send.at[i], recv_sem=recv.at[i], device_id={"dp": to}, device_id_type=pl.DeviceIdType.MESH
        )

    return [
        copy(0, own, rows(me), nxt),
        copy(1, own, rows(me), prv),
        copy(2, own, rows(me), other),
        copy(3, rows(prv, 0, half), rows(prv, 0, half), nxt),
        copy(4, rows(nxt, half, half), rows(nxt, half, half), prv),
        copy(5, rows(prv), rows(prv), other),
        copy(6, rows(nxt), rows(nxt), other),
        copy(7, rows(opp), rows(opp), other),
        pltpu.make_async_copy(own, rows(me), send.at[8]),
    ]


class Gather:
    def __init__(self, number, units, ticks):
        self.number, self.units, self.ticks = number, units, ticks


def call(body, grid, ins, outs, flops, nbytes, prefetch=0, gather=None, kept=(), vmem=62 * 2**20):
    n_in, n_out, n_kept = prefetch + len(ins), len(outs), len(kept)
    hbm = pl.BlockSpec(memory_space=pl.ANY)
    units = gather.units if gather else []
    specs, shapes, scratch, whole = list(ins) + [hbm] * n_kept, [o for _, o in outs], [], body
    if gather:
        steps = grid[0]

        def whole(*refs):
            owns = [part(r) for r, (_, part, _) in zip(refs[n_in + n_kept:], units)]
            results = refs[n_in + n_kept + len(units):]
            wholes, send, recv = results[n_out:n_out + len(units)], results[-2], results[-1]
            copies = [gather_copies(o, w, send.at[u], recv.at[u]) for u, (o, w) in enumerate(zip(owns, wholes))]
            step = pl.program_id(0)

            def first():
                barrier = pltpu.get_barrier_semaphore()
                for d in place()[1:]:
                    pl.semaphore_signal(barrier, inc=1, device_id={"dp": d}, device_id_type=pl.DeviceIdType.MESH)
                pl.semaphore_wait(barrier, 3)
                for c in copies:
                    for i in (0, 1, 2, 8):
                        c[i].start()

            def second(c):
                c[0].wait_recv()
                c[1].wait_recv()
                for i in (3, 4, 5, 6):
                    c[i].start()

            def third(c):
                c[3].wait_recv()
                c[4].wait_recv()
                c[7].start()

            def last():
                for c in copies:
                    for i in (2, 5, 6, 7):
                        c[i].wait_recv()
                    for i in range(8):
                        c[i].wait_send()
                    c[8].wait()

            pl.when(step == 0)(first)
            for c, (two, three) in zip(copies, gather.ticks):
                pl.when(step == two)(functools.partial(second, c))
                if three < steps:
                    pl.when(step == three)(functools.partial(third, c))
            body(*refs[:n_in], *results[:n_out])

            @pl.when(step == steps - 1)
            def _():
                for c, (_, three) in zip(copies, gather.ticks):
                    if three >= steps:
                        third(c)
                last()

        specs += [hbm] * len(units)
        outs = list(outs) + [(hbm, shape((8 * n, w.shape[-1] if cols is None else cols), BF16)) for w, _, (n, cols) in units]
        shapes = [o for _, o in outs]
        scratch = [pltpu.SemaphoreType.DMA((len(units), 9)), pltpu.SemaphoreType.DMA((len(units), 8))]
        extra = dict(collective_id=gather.number, has_side_effects=True)
    else:
        extra = {}
        if kept:
            def whole(*refs):
                body(*refs[:n_in], *refs[n_in + n_kept:])
    made = pl.pallas_call(
        whole,
        grid_spec=pltpu.PrefetchScalarGridSpec(
            num_scalar_prefetch=prefetch, grid=grid, in_specs=specs, out_specs=[s for s, _ in outs], scratch_shapes=scratch
        ),
        out_shape=shapes,
        input_output_aliases={n_in + i: i for i in range(n_kept)},
        cost_estimate=pl.CostEstimate(flops=flops, bytes_accessed=nbytes, transcendentals=0),
        compiler_params=pltpu.CompilerParams(vmem_limit_bytes=vmem, dimension_semantics=("arbitrary",) * len(grid), **extra),
    )

    def run(*args):
        got = made(*args, *kept, *(u[0] for u in units))
        return got[0] if len(outs) == 1 else got

    return run


def pieces(rows, cols):
    return [(rows // 8, cols)] * 6 + [(rows // 4, cols)]


def by_rows(at, d, half, got=None, bn=1024):
    T, N = d.shape
    rows = at.shape[0] // 2
    h = rows // 8

    def theirs(a_ref, d_ref, o_ref):
        o_ref[...] = dot(a_ref[...], d_ref[...], NN).astype(BF16)

    def mine(a_ref, d_ref, got_ref, *outs):
        t = (dot(a_ref[...], d_ref[...], NN) + got_ref[...].astype(F32)).astype(BF16)
        for i in range(6):
            outs[i][...] = t[i * h:(i + 1) * h, :]
        outs[6][...] = t[6 * h:, :]

    col = lambda j: (0, j)
    ins = [pl.BlockSpec((rows, T), lambda j: (half, 0), pipeline_mode=ONE), pl.BlockSpec((T, bn), col)]
    args, results = [at, d], [(rows, N)]
    if got is not None:
        ins.append(pl.BlockSpec((rows, bn), col))
        args.append(got)
        results = pieces(rows, N)
    outs = [(pl.BlockSpec((r, bn), col), shape((r, N), BF16)) for r, _ in results]
    return call(theirs if got is None else mine, (N // bn,), ins, outs, 2 * rows * T * N, T * N * 2)(*args)


def by_blocks(order, p, d, got=None, parts=1):
    T, D = d.shape
    n, bm = order.shape[0], p.shape[1] // 8
    width, h = bm // parts, bm // 2

    def theirs(order_ref, *refs):
        for c in range(parts):
            refs[-1][c * width:(c + 1) * width, :] = dot(refs[c][...], refs[parts][...], TN).astype(BF16)

    def mine(order_ref, *refs):
        outs, step = refs[parts + 2:], pl.program_id(0)
        for c in range(parts):
            r = slice(c * width, (c + 1) * width)
            t = dot(refs[c][...], refs[parts][...], TN)
            refs[parts + 1][r, :] = (t + refs[parts + 1][r, :].astype(F32)).astype(BF16)
        for i in range(3):
            @pl.when(step == i)
            def _():
                outs[2 * i][...] = refs[parts + 1][:h, :]
                outs[2 * i + 1][...] = refs[parts + 1][h:, :]

        @pl.when(step == 3)
        def _():
            outs[6][...] = refs[parts + 1][...]

    ins = [pl.BlockSpec((T, width), functools.partial(lambda c, i, o: (0, c * 8 + o[i]), c)) for c in range(parts)]
    ins.append(pl.BlockSpec((T, D), lambda i, o: (0, 0), pipeline_mode=ONE))
    args = [order, *[p] * parts, d]
    block = pl.BlockSpec((bm, D), lambda i, o: (i, 0))
    outs = [(block, shape((n * bm, D), BF16))]
    if got is not None:
        ins.append(block)
        args.append(got)
        outs = [(pl.BlockSpec(s, lambda i, o: (0, 0)), shape(s, BF16)) for s in pieces(n * bm, D)]
    return call(theirs if got is None else mine, (n,), ins, outs, 2 * n * bm * T * D, T * n * bm * 2, prefetch=1)(*args)


def sent(t, pairs):
    return lax.ppermute(t, "dp", pairs)


def gateup(a, wg, wu, gather, bn=256, bm=512):
    T, D = a.shape
    N = wg.shape[1]

    def body(a_ref, wg_ref, wu_ref, p_ref, u_ref, g_ref):
        for i in range(T // bm):
            r = slice(i * bm, (i + 1) * bm)
            gate = dot(a_ref[r, :], wg_ref[...], NN)
            up = dot(a_ref[r, :], wu_ref[...], NN)
            s = jax.nn.sigmoid(gate)
            silu = gate * s
            p_ref[r, :] = (silu * up).astype(BF16)
            u_ref[r, :] = silu
            g_ref[r, :] = up * (0.5 * (s + silu * (1 - s)))

    col = lambda j: (0, j)
    w, o = pl.BlockSpec((D, bn), col), pl.BlockSpec((T, bn), col)
    return call(
        body, (N // bn,), [pl.BlockSpec((T, D), lambda j: (0, 0), pipeline_mode=ONE), w, w],
        [(o, shape((T, N), BF16)), (o, shape((T, N), F32)), (o, shape((T, N), F32))], 4 * T * D * N, T * N * 10, gather=gather,
    )(a, wg, wu)


def dproduct(dy, wd, by_u, by_g, bm=256, bn=1024):
    T, D = dy.shape
    N = wd.shape[0]

    def body(d_ref, w_ref, u_ref, g_ref, du_ref, dg_ref):
        for i in range(N // bn):
            r = slice(i * bn, (i + 1) * bn)
            dp = dot(d_ref[...], w_ref[r, :], NT).astype(BF16).astype(F32)
            du_ref[:, r] = (dp * u_ref[:, r]).astype(BF16)
            dg_ref[:, r] = (dp * g_ref[:, r] * 2.0).astype(BF16)

    row = lambda j: (j, 0)
    o = pl.BlockSpec((bm, N), row)
    return call(
        body, (T // bm,), [pl.BlockSpec((bm, D), row), pl.BlockSpec((N, D), lambda j: (0, 0), pipeline_mode=ONE), o, o],
        [(o, shape((T, N), BF16)), (o, shape((T, N), BF16))], 2 * T * D * N, T * N * 12,
    )(dy, wd, by_u, by_g)


def both(a, dy, wg, wu, wd, start, gather, kept, bn=256, bm=256):
    T, D = a.shape
    N = wg.shape[1]

    def body(a_ref, d_ref, wg_ref, wu_ref, wd_ref, p_ref, du_ref, dg_ref):
        for i in range(T // bm):
            r = slice(i * bm, (i + 1) * bm)
            gate = dot(a_ref[r, :], wg_ref[...], NN)
            up = dot(a_ref[r, :], wu_ref[...], NN)
            dp = dot(d_ref[r, :], wd_ref[...], NT).astype(BF16).astype(F32)
            s = jax.nn.sigmoid(gate)
            silu = gate * s
            p_ref[r, :] = (silu * up).astype(BF16)
            du_ref[r, :] = (dp * silu).astype(BF16)
            dg_ref[r, :] = (dp * up * (s + silu * (1 - s))).astype(BF16)

    col = lambda j: (0, j)
    full = pl.BlockSpec((T, D), lambda j: (0, 0), pipeline_mode=ONE)
    w, o = pl.BlockSpec((D, bn), col), pl.BlockSpec((T, bn), lambda j: (0, start // bn + j))
    return call(
        body, (N // bn,), [full, full, w, w, pl.BlockSpec((bn, D), lambda j: (start // bn + j, 0))],
        [(o, shape((T, wd.shape[0]), BF16))] * 3, 6 * T * D * N, T * N * 6, gather=gather, kept=kept,
    )(a, dy, wg, wu, wd)


def dnormed(dg, wgs, du, wus, h, g, start, steps, kept, bm=256):
    n = len(wgs)
    T, K = dg.shape
    D = wgs[0].shape[0]

    def product(d_ref, refs):
        total, at = None, 0
        for r in refs:
            t = dot(d_ref[:, at:at + r.shape[1]], r[...], NT)
            total, at = t if total is None else total + t, at + r.shape[1]
        return total.astype(BF16)

    def body(dg_ref, du_ref, *refs):
        h_ref, g_ref, o_ref = refs[2 * n:]
        da = (product(dg_ref, refs[:n]) + product(du_ref, refs[n:2 * n])).astype(F32)
        wide = h_ref[...].astype(F32)
        scale = lax.rsqrt(jnp.mean(wide**2, -1, keepdims=True) + 1e-6)
        inner = jnp.mean(da * wide, -1, keepdims=True)
        o_ref[...] = g_ref[...] + (da * scale - wide * (scale * scale * scale * inner)).astype(BF16)

    row = lambda i: (start + i, 0)
    full = [pl.BlockSpec(w.shape, lambda i: (0, 0), pipeline_mode=ONE) for w in (*wgs, *wus)]
    d, o = pl.BlockSpec((bm, K), row), pl.BlockSpec((bm, D), row)
    return call(
        body, (steps,), [d, d, *full, o, o], [(o, shape((T, D), BF16))], 4 * steps * bm * K * D, steps * bm * K * 4, kept=kept,
    )(dg, du, *wgs, *wus, h, g)


def down(p, w, h, gather, bm=256):
    T, K = p.shape
    D = w.shape[1]

    def body(p_ref, w_ref, h_ref, o_ref):
        o_ref[...] = h_ref[...] + dot(p_ref[...], w_ref[...], NN).astype(BF16)

    row = lambda i: (i, 0)
    o = pl.BlockSpec((bm, D), row)
    return call(
        body, (T // bm,), [pl.BlockSpec((bm, K), row), pl.BlockSpec((K, D), lambda i: (0, 0), pipeline_mode=ONE), o],
        [(o, shape((T, D), BF16))], 2 * T * K * D, T * K * 2, gather=gather,
    )(p, w, h)


def normed(h, gather=None, bm=256):
    T, D = h.shape
    b = D // 8

    def body(h_ref, o_ref, t_ref):
        wide = h_ref[...].astype(F32)
        scale = lax.rsqrt(jnp.mean(wide**2, -1, keepdims=True) + 1e-6)
        o_ref[...] = (wide * scale).astype(BF16)
        me, nxt, prv, _ = place()
        opp = 6 - me + 2 * (me % 2)
        for i, d in enumerate((opp, prv, nxt, me)):
            for j, block in ((i, d + 1 - 2 * (d % 2)), (i + 4, d)):
                t_ref[j * b:(j + 1) * b, :] = o_ref[:, pl.ds(pl.multiple_of(block * b, b), b)].T

    o = pl.BlockSpec((bm, D), lambda i: (i, 0))
    return call(
        body, (T // bm,), [o], [(o, shape((T, D), BF16)), (pl.BlockSpec((D, bm), lambda i: (0, i)), shape((D, T), BF16))],
        T * D * 8, T * D * 6, gather=gather,
    )(h)


def after(t, *before):
    return lax.optimization_barrier((t, *before))[0]


def started(s):
    oa, ob, la, lb, ra, rb, own = s
    return (sent(oa, RIGHT), sent(ob, LEFT), sent(rb, RIGHT), sent(la, LEFT), ra, lb, own)


def joined(s, *before):
    from_left, from_right, far_l, far_r, ra, lb, own, *_ = lax.optimization_barrier((*s, *before))
    to_right = (ra.astype(F32) + from_left.astype(F32)).astype(BF16)
    to_left = (lb.astype(F32) + from_right.astype(F32)).astype(BF16)
    return (to_right, to_left), (sent(to_right, RIGHT), sent(to_left, LEFT), far_l, far_r, own)


def ended(s, *before):
    near_l, near_r, far_l, far_r, own, *_ = lax.optimization_barrier((*s, *before))
    h = own.shape[0] // 2
    top = own[:h].astype(F32) + near_l.astype(F32) + far_r.astype(F32)
    low = own[h:].astype(F32) + far_l.astype(F32) + near_r.astype(F32)
    return jnp.concatenate([top, low]).astype(BF16)


PARTS = (2560, 2304, 1280)


def solution(mesh):
    def body(x, dy, wg, wu, wd):
        order = jnp.asarray(ORDER, jnp.int32)[lax.axis_index("dp")]
        theirs, mine = order[:4], order[4:]
        h0, dy = x[0], dy[0]
        n, FF = wg.shape[1], wg.shape[2]
        own = FF // 8
        offsets = [sum(PARTS[:c]) for c in range(len(PARTS))]
        first, second = lambda r: r.at[0], lambda r: r.at[1]
        cols = lambda c: lambda r: r.at[1, :, pl.ds(offsets[c], PARTS[c])]
        gu = lambda c: [(w, cols(c), (n, PARTS[c])) for w in (wg, wu)]
        a0, at0, wg0, wu0 = normed(h0, Gather(0, [(wg, first, (n, None)), (wu, first, (n, None))], [(7, 8), (7, 8)]))
        act0, u0, g0, wd0, *w1 = gateup(a0, wg0, wu0, Gather(1, [(wd, first, (own, None)), *gu(0)], [(14, 24), (20, 24), (23, 24)]))
        h1, wd1 = down(act0, wd0, h0, Gather(2, [(wd, second, (own, None))], [(7, 8)]))
        a1, at1 = normed(h1)
        act1, du, dg, *w2 = both(a1, dy, *w1, wd1, offsets[0], Gather(3, gu(1), [(3, 8), (6, 10)]), ())
        act1, du, dg, *w3 = both(a1, dy, *w2, wd1, offsets[1], Gather(4, gu(2), [(2, 5), (4, 6)]), (act1, du, dg))
        act1, du, dg = both(a1, dy, *w3, wd1, offsets[2], None, (act1, du, dg))
        wgs, wus = [w1[0], w2[0], w3[0]], [w1[1], w2[1], w3[1]]

        pd = by_blocks(theirs, act1, dy)
        xd = sent(pd, ACROSS)
        pg = by_rows(at1, after(dg, pd), 0)
        xg = sent(pg, ACROSS)
        sd = by_blocks(mine, act1, after(dy, pg), xd)
        rd = started(sd)
        pu = by_rows(at1, after(du, *sd), 0)
        xu = sent(pu, ACROSS)
        sg = by_rows(at1, after(dg, pu), 1, xg)
        rg = started(sg)
        jd, rd = joined(rd, *sg)
        su = by_rows(at1, after(du, *jd), 1, xu)
        ru = started(su)
        part = dnormed(after(dg, *su), wgs, du, wus, h1, dy, 0, 4, ())
        jg, rg = joined(rg, part)
        dwd1 = ended(rd, part)
        d1 = dnormed(after(dg, part, dwd1, *jg), wgs, du, wus, h1, dy, 4, 4, (part,))
        ju, ru = joined(ru, d1)
        d1 = after(d1, *ju)
        pd = by_blocks(theirs, act0, d1)
        xd = sent(pd, ACROSS)
        dwg1 = ended(rg, pd)

        du, dg = dproduct(after(d1, pd, dwg1), wd0, u0, g0)
        dwu1 = ended(ru, dg)
        sd = by_blocks(mine, act0, after(d1, dg, dwu1), xd)
        rd = started(sd)
        pg = by_rows(at0, after(dg, *sd), 0)
        xg = sent(pg, ACROSS)
        pu = by_rows(at0, after(du, pg), 0)
        xu = sent(pu, ACROSS)
        jd, rd = joined(rd, pu)
        sg = by_rows(at0, after(dg, *jd), 1, xg)
        rg = started(sg)
        su = by_rows(at0, after(du, *sg), 1, xu)
        ru = started(su)
        dwd0 = ended(rd, *su)
        dwd = jnp.stack([dwd0, dwd1])
        part = dnormed(after(dg, dwd, *su), [wg0], du, [wu0], h0, d1, 0, 5, ())
        jg, rg = joined(rg, part)
        ju, ru = joined(ru, part)
        d0 = dnormed(after(dg, part, *jg, *ju), [wg0], du, [wu0], h0, d1, 5, 3, (part,))
        dwg0, dwu0 = ended(rg, d0), ended(ru, d0)
        return d0[None], jnp.stack([dwg0, dwg1]), jnp.stack([dwu0, dwu1]), dwd

    data, rows = P(("rep", "dp"), None, None), P(None, "dp", None)
    out = P("rep", "dp", None)
    return jax.shard_map(body, mesh=mesh, in_specs=(data, data, rows, rows, rows), out_specs=(data, out, out, out), check_vma=False)
```

```python
import functools

import jax
import jax.numpy as jnp
from jax import lax
from jax.experimental import pallas as pl
from jax.experimental.pallas import tpu as pltpu
from jax.sharding import PartitionSpec as P


F32, BF16 = jnp.float32, jnp.bfloat16
NN = (((1,), (0,)), ((), ()))
NT = (((1,), (1,)), ((), ()))
TN = (((0,), (0,)), ((), ()))
ONE = pl.Buffered(1)

NEXT = (1, 3, 0, 2)
PREV = (2, 0, 3, 1)
RIGHT = [(2 * c + k, 2 * NEXT[c] + k) for c in range(4) for k in range(2)]
LEFT = [(2 * c + k, 2 * PREV[c] + k) for c in range(4) for k in range(2)]
ACROSS = [(d, d ^ 1) for d in range(8)]
ORDER = [[2 * chip + core for core in (1 - k, k) for chip in (3 - c, PREV[c], NEXT[c], c)] for c in range(4) for k in range(2)]


def dot(a, b, dims):
    return lax.dot_general(a, b, dims, preferred_element_type=F32)


def shape(dims, dtype):
    return jax.ShapeDtypeStruct(dims, dtype)


def place():
    me = lax.axis_index("dp")
    x, y, k = me // 4, (me // 2) % 2, me % 2
    return me, (2 * y + 1 - x) * 2 + k, (2 * (1 - y) + x) * 2 + k, me + 1 - 2 * k


def gather_copies(own, whole, send, recv):
    me, nxt, prv, other = place()
    n = whole.shape[0] // 8
    half = n // 2
    rows = lambda d, start=0, size=n: whole.at[pl.ds(pl.multiple_of(d * n + start, 8), size)]
    opp = 6 - me + 2 * (me % 2)

    def copy(i, src, dst, to):
        return pltpu.make_async_remote_copy(
            src_ref=src, dst_ref=dst, send_sem=send.at[i], recv_sem=recv.at[i], device_id={"dp": to}, device_id_type=pl.DeviceIdType.MESH
        )

    return [
        copy(0, own, rows(me), nxt),
        copy(1, own, rows(me), prv),
        copy(2, own, rows(me), other),
        copy(3, rows(prv, 0, half), rows(prv, 0, half), nxt),
        copy(4, rows(nxt, half, half), rows(nxt, half, half), prv),
        copy(5, rows(prv), rows(prv), other),
        copy(6, rows(nxt), rows(nxt), other),
        copy(7, rows(opp), rows(opp), other),
        pltpu.make_async_copy(own, rows(me), send.at[8]),
    ]


class Gather:
    def __init__(self, number, units, ticks):
        self.number, self.units, self.ticks = number, units, ticks


def call(body, grid, ins, outs, flops, nbytes, prefetch=0, gather=None, kept=(), scratch=(), sums=(), vmem=62 * 2**20):
    n_in, n_out, n_kept, n_main = prefetch + len(ins), len(outs), len(kept), len(outs)
    added = [t for terms in sums for t in terms]
    hbm = pl.BlockSpec(memory_space=pl.ANY)
    units = gather.units if gather else []
    specs, shapes, scratch, whole = list(ins) + [hbm] * n_kept, [o for _, o in outs], list(scratch), body
    if gather:
        steps = grid[0]

        def whole(*refs):
            owns = [part(r) for r, (_, part, _) in zip(refs[n_in + n_kept:], units)]
            results = refs[n_in + n_kept + len(units):]
            wholes, (*mine, send, recv) = results[n_out:n_out + len(units)], results[n_out + len(units):]
            copies = [gather_copies(o, w, send.at[u], recv.at[u]) for u, (o, w) in enumerate(zip(owns, wholes))]
            step = pl.program_id(0)

            def first():
                barrier = pltpu.get_barrier_semaphore()
                for d in place()[1:]:
                    pl.semaphore_signal(barrier, inc=1, device_id={"dp": d}, device_id_type=pl.DeviceIdType.MESH)
                pl.semaphore_wait(barrier, 3)
                for c in copies:
                    for i in (0, 1, 2, 8):
                        c[i].start()

            def second(c):
                c[0].wait_recv()
                c[1].wait_recv()
                for i in (3, 4, 5, 6):
                    c[i].start()

            def third(c):
                c[3].wait_recv()
                c[4].wait_recv()
                c[7].start()

            def last():
                for c in copies:
                    for i in (2, 5, 6, 7):
                        c[i].wait_recv()
                    for i in range(8):
                        c[i].wait_send()
                    c[8].wait()

            pl.when(step == 0)(first)
            for c, (two, three) in zip(copies, gather.ticks):
                pl.when(step == two)(functools.partial(second, c))
                if three < steps:
                    pl.when(step == three)(functools.partial(third, c))
            body(*refs[:n_in], *results[:n_out], *mine)

            @pl.when(step == steps - 1)
            def _():
                for c, (_, three) in zip(copies, gather.ticks):
                    if three >= steps:
                        third(c)
                last()

        specs += [hbm] * len(units)
        outs = list(outs) + [(hbm, shape((8 * n, w.shape[-1] if cols is None else cols), BF16)) for w, _, (n, cols) in units]
        shapes = [o for _, o in outs]
        scratch += [pltpu.SemaphoreType.DMA((len(units), 9)), pltpu.SemaphoreType.DMA((len(units), 8))]
        extra = dict(collective_id=gather.number, has_side_effects=True)
    else:
        extra = {}
        steps = grid[0]

        def piece(t):
            r, c = t.shape
            if c % (128 * steps) == 0:
                return pl.BlockSpec((r, c // steps), lambda j, *_: (0, j))
            return pl.BlockSpec((r // steps, c), lambda j, *_: (j, 0))

        specs += [piece(t) for t in added]
        outs = list(outs) + [(piece(terms[0]), shape(terms[0].shape, BF16)) for terms in sums]
        shapes = [o for _, o in outs]

        def whole(*refs):
            terms = refs[n_in + n_kept:]
            results = terms[len(added):]
            at = 0
            for o_ref, group in zip(results[n_main:], sums):
                total = terms[at][...].astype(F32)
                for t in terms[at + 1:at + len(group)]:
                    total = total + t[...].astype(F32)
                o_ref[...] = total.astype(BF16)
                at += len(group)
            body(*refs[:n_in], *results[:n_main], *results[n_main + len(sums):])
    made = pl.pallas_call(
        whole,
        grid_spec=pltpu.PrefetchScalarGridSpec(
            num_scalar_prefetch=prefetch, grid=grid, in_specs=specs, out_specs=[s for s, _ in outs], scratch_shapes=scratch
        ),
        out_shape=shapes,
        input_output_aliases={n_in + i: i for i in range(n_kept)},
        cost_estimate=pl.CostEstimate(flops=flops, bytes_accessed=nbytes, transcendentals=0),
        compiler_params=pltpu.CompilerParams(vmem_limit_bytes=vmem, dimension_semantics=("arbitrary",) * len(grid), **extra),
    )

    def run(*args):
        got = made(*args, *kept, *added, *(u[0] for u in units))
        return got[0] if len(outs) == 1 else got

    return run


def pieces(rows, cols):
    return [(rows // 8, cols)] * 8


def by_rows(at, d, half, got=None, bn=1024, sums=()):
    T, N = d.shape
    rows = at.shape[0] // 2
    h = rows // 8

    def theirs(a_ref, d_ref, o_ref):
        o_ref[...] = dot(a_ref[...], d_ref[...], NN).astype(BF16)

    def mine(a_ref, d_ref, got_ref, *outs):
        t = (dot(a_ref[...], d_ref[...], NN) + got_ref[...].astype(F32)).astype(BF16)
        for i in range(8):
            outs[i][...] = t[i * h:(i + 1) * h, :]

    col = lambda j: (0, j)
    ins = [pl.BlockSpec((rows, T), lambda j: (half, 0), pipeline_mode=ONE), pl.BlockSpec((T, bn), col)]
    args, results = [at, d], [(rows, N)]
    if got is not None:
        ins.append(pl.BlockSpec((rows, bn), col))
        args.append(got)
        results = pieces(rows, N)
    outs = [(pl.BlockSpec((r, bn), col), shape((r, N), BF16)) for r, _ in results]
    return call(theirs if got is None else mine, (N // bn,), ins, outs, 2 * rows * T * N, T * N * 2, sums=sums)(*args)


def by_blocks(order, p, d, got=None, parts=1, sums=()):
    T, D = d.shape
    n, bm = order.shape[0], p.shape[1] // 8
    width, h = bm // parts, bm // 2

    def theirs(order_ref, *refs):
        for c in range(parts):
            refs[-1][c * width:(c + 1) * width, :] = dot(refs[c][...], refs[parts][...], TN).astype(BF16)

    def mine(order_ref, *refs):
        outs, step = refs[parts + 2:], pl.program_id(0)
        for c in range(parts):
            r = slice(c * width, (c + 1) * width)
            t = dot(refs[c][...], refs[parts][...], TN)
            refs[parts + 1][r, :] = (t + refs[parts + 1][r, :].astype(F32)).astype(BF16)
        for i in range(4):
            @pl.when(step == i)
            def _():
                outs[2 * i][...] = refs[parts + 1][:h, :]
                outs[2 * i + 1][...] = refs[parts + 1][h:, :]

    ins = [pl.BlockSpec((T, width), functools.partial(lambda c, i, o: (0, c * 8 + o[i]), c)) for c in range(parts)]
    ins.append(pl.BlockSpec((T, D), lambda i, o: (0, 0), pipeline_mode=ONE))
    args = [order, *[p] * parts, d]
    block = pl.BlockSpec((bm, D), lambda i, o: (i, 0))
    outs = [(block, shape((n * bm, D), BF16))]
    if got is not None:
        ins.append(block)
        args.append(got)
        outs = [(pl.BlockSpec(s, lambda i, o: (0, 0)), shape(s, BF16)) for s in pieces(n * bm, D)]
    return call(
        theirs if got is None else mine, (n,), ins, outs, 2 * n * bm * T * D, T * n * bm * 2, prefetch=1, sums=sums
    )(*args)


def sent(t, pairs):
    return lax.ppermute(t, "dp", pairs)


def gateup(a, wg, wu, gather, bn=256, bm=512):
    T, D = a.shape
    N = wg.shape[1]

    def body(a_ref, wg_ref, wu_ref, p_ref, u_ref, g_ref):
        for i in range(T // bm):
            r = slice(i * bm, (i + 1) * bm)
            gate = dot(a_ref[r, :], wg_ref[...], NN)
            up = dot(a_ref[r, :], wu_ref[...], NN)
            s = jax.nn.sigmoid(gate)
            silu = gate * s
            p_ref[r, :] = (silu * up).astype(BF16)
            u_ref[r, :] = silu
            g_ref[r, :] = up * (0.5 * (s + silu * (1 - s)))

    col = lambda j: (0, j)
    w, o = pl.BlockSpec((D, bn), col), pl.BlockSpec((T, bn), col)
    return call(
        body, (N // bn,), [pl.BlockSpec((T, D), lambda j: (0, 0), pipeline_mode=ONE), w, w],
        [(o, shape((T, N), BF16)), (o, shape((T, N), F32)), (o, shape((T, N), F32))], 4 * T * D * N, T * N * 10, gather=gather,
    )(a, wg, wu)


def loaded(sources, targets, sems):
    copies = [pltpu.make_async_copy(s, t, sems.at[i]) for i, (s, t) in enumerate(zip(sources, targets))]
    for c in copies:
        c.start()
    return lambda i: copies[i].wait()


def dproduct(dy, wd, by_u, by_g, bm=256, bn=1024):
    T, D = dy.shape
    N = wd.shape[0]
    n = N // bn

    def body(d_ref, w_hbm, u_ref, g_ref, du_ref, dg_ref, w_ref, sems):
        def all_of(wait):
            for i in range(n):
                wait(i)
                r = slice(i * bn, (i + 1) * bn)
                dp = dot(d_ref[...], w_ref[r, :], NT).astype(BF16).astype(F32)
                du_ref[:, r] = (dp * u_ref[:, r]).astype(BF16)
                dg_ref[:, r] = (dp * g_ref[:, r] * 2.0).astype(BF16)

        @pl.when(pl.program_id(0) == 0)
        def _():
            cuts = [pl.ds(i * bn, bn) for i in range(n)]
            all_of(loaded([w_hbm.at[c] for c in cuts], [w_ref.at[c] for c in cuts], sems))

        @pl.when(pl.program_id(0) != 0)
        def _():
            all_of(lambda i: None)

    row = lambda j: (j, 0)
    o = pl.BlockSpec((bm, N), row)
    return call(
        body, (T // bm,), [pl.BlockSpec((bm, D), row), pl.BlockSpec(memory_space=pl.ANY), o, o],
        [(o, shape((T, N), BF16)), (o, shape((T, N), BF16))], 2 * T * D * N, T * N * 12,
        scratch=[pltpu.VMEM((N, D), BF16), pltpu.SemaphoreType.DMA((n,))],
    )(dy, wd, by_u, by_g)


def both(a, dy, wg, wu, wd, start, gather, kept, bn=256, bm=256):
    T, D = a.shape
    N = wg.shape[1]

    def body(a_ref, d_ref, wg_ref, wu_ref, wd_ref, p_ref, du_ref, dg_ref):
        for i in range(T // bm):
            r = slice(i * bm, (i + 1) * bm)
            gate = dot(a_ref[r, :], wg_ref[...], NN)
            up = dot(a_ref[r, :], wu_ref[...], NN)
            dp = dot(d_ref[r, :], wd_ref[...], NT).astype(BF16).astype(F32)
            s = jax.nn.sigmoid(gate)
            silu = gate * s
            p_ref[r, :] = (silu * up).astype(BF16)
            du_ref[r, :] = (dp * silu).astype(BF16)
            dg_ref[r, :] = (dp * up * (s + silu * (1 - s))).astype(BF16)

    col = lambda j: (0, j)
    full = pl.BlockSpec((T, D), lambda j: (0, 0), pipeline_mode=ONE)
    w, o = pl.BlockSpec((D, bn), col), pl.BlockSpec((T, bn), lambda j: (0, start // bn + j))
    return call(
        body, (N // bn,), [full, full, w, w, pl.BlockSpec((bn, D), lambda j: (start // bn + j, 0))],
        [(o, shape((T, wd.shape[0]), BF16))] * 3, 6 * T * D * N, T * N * 6, gather=gather, kept=kept,
    )(a, dy, wg, wu, wd)


def dnormed(dg, wgs, du, wus, h, g, start, steps, kept, sums=(), bm=256):
    n = len(wgs)
    T, K = dg.shape
    D = wgs[0].shape[0]
    cuts, at = [], 0
    for p, w in enumerate(wgs):
        each = next(c for c in (1280, 1152, 1024) if w.shape[1] % c == 0)
        for i in range(w.shape[1] // each):
            cuts.append((p, i * each, at + i * each, each))
        at += w.shape[1]

    def body(dg_ref, du_ref, *refs):
        h_ref, g_ref, o_ref, wg_ref, wu_ref, da_ref, sems = refs[2 * n:]

        @pl.when(pl.program_id(0) == 0)
        def _():
            sources = [refs[m * n + p].at[:, pl.ds(c, w)] for m in range(2) for p, c, _, w in cuts]
            targets = [r.at[:, pl.ds(c, w)] for r in (wg_ref, wu_ref) for _, _, c, w in cuts]
            wait = loaded(sources, targets, sems)
            sums = []
            for m, (d_ref, w_ref) in enumerate(((dg_ref, wg_ref), (du_ref, wu_ref))):
                total = None
                for i, (_, _, c, w) in enumerate(cuts):
                    wait(m * len(cuts) + i)
                    t = dot(d_ref[:, c:c + w], w_ref[:, c:c + w], NT)
                    total = t if total is None else total + t
                sums.append(total.astype(BF16))
            da_ref[...] = sums[0] + sums[1]

        @pl.when(pl.program_id(0) != 0)
        def _():
            da_ref[...] = dot(dg_ref[...], wg_ref[...], NT).astype(BF16) + dot(du_ref[...], wu_ref[...], NT).astype(BF16)

        da, wide = da_ref[...].astype(F32), h_ref[...].astype(F32)
        scale = lax.rsqrt(jnp.mean(wide**2, -1, keepdims=True) + 1e-6)
        inner = jnp.mean(da * wide, -1, keepdims=True)
        o_ref[...] = g_ref[...] + (da * scale - wide * (scale * scale * scale * inner)).astype(BF16)

    row = lambda i: (start + i, 0)
    d, o = pl.BlockSpec((bm, K), row), pl.BlockSpec((bm, D), row)
    return call(
        body, (steps,), [d, d, *[pl.BlockSpec(memory_space=pl.ANY)] * (2 * n), o, o], [(o, shape((T, D), BF16))],
        4 * steps * bm * K * D, steps * bm * K * 4, kept=kept, sums=sums,
        scratch=[pltpu.VMEM((D, K), BF16)] * 2 + [pltpu.VMEM((bm, D), BF16), pltpu.SemaphoreType.DMA((2 * len(cuts),))],
    )(dg, du, *wgs, *wus, h, g)


def down(p, w, h, gather, bm=256, bk=1024):
    T, K = p.shape
    D = w.shape[1]
    n = K // bk

    def body(p_ref, w_hbm, h_ref, o_ref, w_ref, sems):
        @pl.when(pl.program_id(0) == 0)
        def _():
            cuts = [pl.ds(i * bk, bk) for i in range(n)]
            wait = loaded([w_hbm.at[c] for c in cuts], [w_ref.at[c] for c in cuts], sems)
            total = None
            for i in range(n):
                wait(i)
                t = dot(p_ref[:, i * bk:(i + 1) * bk], w_ref[i * bk:(i + 1) * bk, :], NN)
                total = t if total is None else total + t
            o_ref[...] = h_ref[...] + total.astype(BF16)

        @pl.when(pl.program_id(0) != 0)
        def _():
            o_ref[...] = h_ref[...] + dot(p_ref[...], w_ref[...], NN).astype(BF16)

    row = lambda i: (i, 0)
    o = pl.BlockSpec((bm, D), row)
    return call(
        body, (T // bm,), [pl.BlockSpec((bm, K), row), pl.BlockSpec(memory_space=pl.ANY), o],
        [(o, shape((T, D), BF16))], 2 * T * K * D, T * K * 2, gather=gather,
        scratch=[pltpu.VMEM((K, D), BF16), pltpu.SemaphoreType.DMA((n,))],
    )(p, w, h)


def normed(h, gather=None, bm=256):
    T, D = h.shape
    b = D // 8

    def body(h_ref, o_ref, t_ref):
        wide = h_ref[...].astype(F32)
        scale = lax.rsqrt(jnp.mean(wide**2, -1, keepdims=True) + 1e-6)
        o_ref[...] = (wide * scale).astype(BF16)
        me, nxt, prv, _ = place()
        opp = 6 - me + 2 * (me % 2)
        for i, d in enumerate((opp, prv, nxt, me)):
            for j, block in ((i, d + 1 - 2 * (d % 2)), (i + 4, d)):
                t_ref[j * b:(j + 1) * b, :] = o_ref[:, pl.ds(pl.multiple_of(block * b, b), b)].T

    o = pl.BlockSpec((bm, D), lambda i: (i, 0))
    return call(
        body, (T // bm,), [o], [(o, shape((T, D), BF16)), (pl.BlockSpec((D, bm), lambda i: (0, i)), shape((D, T), BF16))],
        T * D * 8, T * D * 6, gather=gather,
    )(h)


def after(t, *before):
    return lax.optimization_barrier((t, *before))[0]


def started(s):
    oa, ob, la, lb, ra, rb, top, low = s
    got = [sent(oa, RIGHT), sent(ob, LEFT), sent(rb, RIGHT), sent(la, LEFT)]
    return (*got, ra, lb, top, low)


def joins(s):
    from_left, from_right, _, _, ra, lb, _, _ = s
    return [(ra, from_left), (lb, from_right)]


def on(s, to_right, to_left):
    _, _, far_l, far_r, _, _, top, low = s
    near_l, near_r = sent(to_right, RIGHT), sent(to_left, LEFT)
    return [(top, near_l, far_r), (low, far_l, near_r)]


def ended(sums):
    h, c = sums[0][0].shape
    terms = [t for group in sums for t in group]

    def body(*refs):
        at = 0
        for i, group in enumerate(sums):
            total = refs[at][...].astype(F32)
            for t in refs[at + 1:at + len(group)]:
                total = total + t[...].astype(F32)
            refs[-1][i // 2, i % 2 * h:(i % 2 + 1) * h, :] = total.astype(BF16)
            at += len(group)

    col = c // 4
    return call(
        body, (4,), [pl.BlockSpec((h, col), lambda j: (0, j))] * len(terms),
        [(pl.BlockSpec((len(sums) // 2, 2 * h, col), lambda j: (0, 0, j)), shape((len(sums) // 2, 2 * h, c), BF16))], h * c * 8, h * c * 24,
    )(*terms)


def summed(sums):
    n = sum(t.size for terms in sums for t in terms)
    return call(lambda *refs: None, (4,), [], [], n, n * 4, sums=sums)()


PARTS = (2560, 2304, 1280)


def solution(mesh):
    def body(x, dy, wg, wu, wd):
        order = jnp.asarray(ORDER, jnp.int32)[lax.axis_index("dp")]
        theirs, mine = order[:4], order[4:]
        h0, dy = x[0], dy[0]
        n, FF = wg.shape[1], wg.shape[2]
        own = FF // 8
        offsets = [sum(PARTS[:c]) for c in range(len(PARTS))]
        first, second = lambda r: r.at[0], lambda r: r.at[1]
        cols = lambda c: lambda r: r.at[1, :, pl.ds(offsets[c], PARTS[c])]
        gu = lambda c: [(w, cols(c), (n, PARTS[c])) for w in (wg, wu)]
        a0, at0, wg0, wu0 = normed(h0, Gather(0, [(wg, first, (n, None)), (wu, first, (n, None))], [(7, 8), (7, 8)]))
        act0, u0, g0, wd0, *w1 = gateup(a0, wg0, wu0, Gather(1, [(wd, first, (own, None)), *gu(0)], [(14, 24), (20, 24), (23, 24)]))
        h1, wd1 = down(act0, wd0, h0, Gather(2, [(wd, second, (own, None))], [(7, 8)]))
        a1, at1 = normed(h1)
        act1, du, dg, *w2 = both(a1, dy, *w1, wd1, offsets[0], Gather(3, gu(1), [(3, 8), (6, 10)]), ())
        act1, du, dg, *w3 = both(a1, dy, *w2, wd1, offsets[1], Gather(4, gu(2), [(2, 5), (4, 6)]), (act1, du, dg))
        act1, du, dg = both(a1, dy, *w3, wd1, offsets[2], None, (act1, du, dg))
        wgs, wus = [w1[0], w2[0], w3[0]], [w1[1], w2[1], w3[1]]

        pd = by_blocks(theirs, act1, dy)
        xd = sent(pd, ACROSS)
        pg = by_rows(at1, after(dg, pd), 0)
        xg = sent(pg, ACROSS)
        sd = by_blocks(mine, act1, after(dy, pg), xd)
        rd = started(sd)
        pu = by_rows(at1, after(du, *sd), 0)
        xu = sent(pu, ACROSS)
        sg = by_rows(at1, after(dg, pu), 1, xg)
        rg = started(sg)
        *su, jr, jl = by_rows(at1, after(du, *sg), 1, xu, sums=joins(rd))
        ru = started(su)
        ed = on(rd, jr, jl)
        d1 = dnormed(after(dg, *su), wgs, du, wus, h1, dy, 0, 8, ())
        pd, gr, gl, ur, ul, *dwd1 = by_blocks(theirs, act0, d1, sums=[*joins(rg), *joins(ru), *ed])
        xd = sent(pd, ACROSS)
        eg, eu = on(rg, gr, gl), on(ru, ur, ul)

        du, dg = dproduct(after(d1, pd), wd0, u0, g0)
        *sd, gt, gb, ut, ub = by_blocks(mine, act0, after(d1, dg), xd, sums=[*eg, *eu])
        rd = started(sd)
        pg = by_rows(at0, after(dg, *sd), 0)
        xg = sent(pg, ACROSS)
        pu = by_rows(at0, after(du, pg), 0)
        xu = sent(pu, ACROSS)
        *sg, jr, jl = by_rows(at0, after(dg, pu), 1, xg, sums=joins(rd))
        rg = started(sg)
        ed = on(rd, jr, jl)
        su = by_rows(at0, after(du, *sg), 1, xu)
        ru = started(su)
        part = dnormed(after(dg, *su), [wg0], du, [wu0], h0, d1, 0, 6, ())
        _, jg, ju = lax.optimization_barrier((part, joins(rg), joins(ru)))
        sums = summed([*jg, *ju])
        g2, u2 = sums[:2], sums[2:]
        eg, eu = on(rg, *g2), on(ru, *u2)
        d0, *dwd0 = dnormed(after(dg, part, *g2, *u2), [wg0], du, [wu0], h0, d1, 6, 2, (part,), sums=ed)
        dwd = jnp.stack([jnp.concatenate(dwd0), jnp.concatenate(dwd1)])
        dwg, dwu = ended([*eg, (gt,), (gb,)]), ended([*eu, (ut,), (ub,)])
        return d0[None], dwg, dwu, dwd

    data, rows = P(("rep", "dp"), None, None), P(None, "dp", None)
    out = P("rep", "dp", None)
    return jax.shard_map(body, mesh=mesh, in_specs=(data, data, rows, rows, rows), out_specs=(data, out, out, out), check_vma=False)
```

```python
import functools

import jax
import jax.numpy as jnp
from jax import lax
from jax.experimental import pallas as pl
from jax.experimental.pallas import tpu as pltpu
from jax.sharding import PartitionSpec as P


F32, BF16 = jnp.float32, jnp.bfloat16
NN = (((1,), (0,)), ((), ()))
NT = (((1,), (1,)), ((), ()))
TN = (((0,), (0,)), ((), ()))
ONE = pl.Buffered(1)

NEXT = (1, 3, 0, 2)
PREV = (2, 0, 3, 1)
RIGHT = [(2 * c + k, 2 * NEXT[c] + k) for c in range(4) for k in range(2)]
LEFT = [(2 * c + k, 2 * PREV[c] + k) for c in range(4) for k in range(2)]
ACROSS = [(d, d ^ 1) for d in range(8)]
ORDER = [[2 * chip + core for core in (1 - k, k) for chip in (3 - c, PREV[c], NEXT[c], c)] for c in range(4) for k in range(2)]


def dot(a, b, dims):
    return lax.dot_general(a, b, dims, preferred_element_type=F32)


def shape(dims, dtype):
    return jax.ShapeDtypeStruct(dims, dtype)


def place():
    me = lax.axis_index("dp")
    x, y, k = me // 4, (me // 2) % 2, me % 2
    return me, (2 * y + 1 - x) * 2 + k, (2 * (1 - y) + x) * 2 + k, me + 1 - 2 * k


def gather_copies(own, whole, send, recv):
    me, nxt, prv, other = place()
    n = whole.shape[0] // 8
    half = n // 2
    rows = lambda d, start=0, size=n: whole.at[pl.ds(pl.multiple_of(d * n + start, 8), size)]
    opp = 6 - me + 2 * (me % 2)

    def copy(i, src, dst, to):
        return pltpu.make_async_remote_copy(
            src_ref=src, dst_ref=dst, send_sem=send.at[i], recv_sem=recv.at[i], device_id={"dp": to}, device_id_type=pl.DeviceIdType.MESH
        )

    return [
        copy(0, own, rows(me), nxt),
        copy(1, own, rows(me), prv),
        copy(2, own, rows(me), other),
        copy(3, rows(prv, 0, half), rows(prv, 0, half), nxt),
        copy(4, rows(nxt, half, half), rows(nxt, half, half), prv),
        copy(5, rows(prv), rows(prv), other),
        copy(6, rows(nxt), rows(nxt), other),
        copy(7, rows(opp), rows(opp), other),
        pltpu.make_async_copy(own, rows(me), send.at[8]),
    ]


class Gather:
    def __init__(self, number, units, ticks):
        self.number, self.units, self.ticks = number, units, ticks


def plane_of(t):
    return t if isinstance(t, tuple) else (t, None)


def call(body, grid, ins, outs, flops, nbytes, prefetch=0, gather=None, kept=(), scratch=(), sums=(), vmem=62 * 2**20):
    n_in, n_out, n_kept, n_main = prefetch + len(ins), len(outs), len(kept), len(outs)
    added = [t for terms in sums for t in terms]
    hbm = pl.BlockSpec(memory_space=pl.ANY)
    units = gather.units if gather else []
    specs, shapes, scratch, whole = list(ins) + [hbm] * n_kept, [o for _, o in outs], list(scratch), body
    if gather:
        steps = grid[0]

        def whole(*refs):
            owns = [part(r) for r, (_, part, _) in zip(refs[n_in + n_kept:], units)]
            results = refs[n_in + n_kept + len(units):]
            wholes, (*mine, send, recv) = results[n_out:n_out + len(units)], results[n_out + len(units):]
            copies = [gather_copies(o, w, send.at[u], recv.at[u]) for u, (o, w) in enumerate(zip(owns, wholes))]
            step = pl.program_id(0)

            def first():
                barrier = pltpu.get_barrier_semaphore()
                for d in place()[1:]:
                    pl.semaphore_signal(barrier, inc=1, device_id={"dp": d}, device_id_type=pl.DeviceIdType.MESH)
                pl.semaphore_wait(barrier, 3)
                for c in copies:
                    for i in (0, 1, 2, 8):
                        c[i].start()

            def second(c):
                c[0].wait_recv()
                c[1].wait_recv()
                for i in (3, 4, 5, 6):
                    c[i].start()

            def third(c):
                c[3].wait_recv()
                c[4].wait_recv()
                c[7].start()

            def last():
                for c in copies:
                    for i in (2, 5, 6, 7):
                        c[i].wait_recv()
                    for i in range(8):
                        c[i].wait_send()
                    c[8].wait()

            pl.when(step == 0)(first)
            for c, (two, three) in zip(copies, gather.ticks):
                pl.when(step == two)(functools.partial(second, c))
                if three < steps:
                    pl.when(step == three)(functools.partial(third, c))
            body(*refs[:n_in], *results[:n_out], *mine)

            @pl.when(step == steps - 1)
            def _():
                for c, (_, three) in zip(copies, gather.ticks):
                    if three >= steps:
                        third(c)
                last()

        specs += [hbm] * len(units)
        outs = list(outs) + [(hbm, shape((8 * n, w.shape[-1] if cols is None else cols), BF16)) for w, _, (n, cols) in units]
        shapes = [o for _, o in outs]
        scratch += [pltpu.SemaphoreType.DMA((len(units), 9)), pltpu.SemaphoreType.DMA((len(units), 8))]
        extra = dict(collective_id=gather.number, has_side_effects=True)
    else:
        extra = {}
        steps = grid[0]

        def piece(t):
            whole, plane = plane_of(t)
            r, c = whole.shape[-2:]
            across = c % (128 * steps) == 0
            block = (r, c // steps) if across else (r // steps, c)
            if plane is None:
                return pl.BlockSpec(block, lambda j, *_: (0, j) if across else (j, 0))
            return pl.BlockSpec((None, *block), lambda j, *_: (plane, 0, j) if across else (plane, j, 0))

        specs += [piece(t) for t in added]
        outs = list(outs) + [(piece(terms[0]), shape(terms[0].shape, BF16)) for terms in sums]
        shapes = [o for _, o in outs]

        def whole(*refs):
            terms = refs[n_in + n_kept:]
            results = terms[len(added):]
            at = 0
            for o_ref, group in zip(results[n_main:], sums):
                total = terms[at][...].astype(F32)
                for t in terms[at + 1:at + len(group)]:
                    total = total + t[...].astype(F32)
                o_ref[...] = total.astype(BF16)
                at += len(group)
            body(*refs[:n_in], *results[:n_main], *results[n_main + len(sums):])
    made = pl.pallas_call(
        whole,
        grid_spec=pltpu.PrefetchScalarGridSpec(
            num_scalar_prefetch=prefetch, grid=grid, in_specs=specs, out_specs=[s for s, _ in outs], scratch_shapes=scratch
        ),
        out_shape=shapes,
        input_output_aliases={n_in + i: i for i in range(n_kept)},
        cost_estimate=pl.CostEstimate(flops=flops, bytes_accessed=nbytes, transcendentals=0),
        compiler_params=pltpu.CompilerParams(vmem_limit_bytes=vmem, dimension_semantics=("arbitrary",) * len(grid), **extra),
    )

    def run(*args):
        got = made(*args, *kept, *(plane_of(t)[0] for t in added), *(u[0] for u in units))
        return got[0] if len(outs) == 1 else got

    return run


PIECES = ((0, 5), (1, 2), (4,), (3,), (6,), (7,))


def pieces(rows, cols):
    return [(len(p), rows // 8, cols) if len(p) > 1 else (rows // 8, cols) for p in PIECES]


def put(outs, half, value):
    for o_ref, p in zip(outs, PIECES):
        if half in p:
            if len(p) > 1:
                o_ref[p.index(half)] = value
            else:
                o_ref[...] = value


def by_rows(at, d, half, got=None, bn=1024, sums=()):
    T, N = d.shape
    rows = at.shape[0] // 2
    h = rows // 8

    def theirs(a_ref, d_ref, o_ref):
        o_ref[...] = dot(a_ref[...], d_ref[...], NN).astype(BF16)

    def mine(a_ref, d_ref, got_ref, *outs):
        t = (dot(a_ref[...], d_ref[...], NN) + got_ref[...].astype(F32)).astype(BF16)
        for i in range(8):
            put(outs, i, t[i * h:(i + 1) * h, :])

    col = lambda j: (0, j)
    ins = [pl.BlockSpec((rows, T), lambda j: (half, 0), pipeline_mode=ONE), pl.BlockSpec((T, bn), col)]
    args, results = [at, d], [(rows, N)]
    if got is not None:
        ins.append(pl.BlockSpec((rows, bn), col))
        args.append(got)
        results = pieces(rows, N)
    outs = [(pl.BlockSpec((*s[:-1], bn), functools.partial(lambda k, j: (0,) * k + (j,), len(s) - 1)), shape(s, BF16)) for s in results]
    return call(theirs if got is None else mine, (N // bn,), ins, outs, 2 * rows * T * N, T * N * 2, sums=sums)(*args)


def by_blocks(order, p, d, got=None, parts=1, sums=()):
    T, D = d.shape
    n, bm = order.shape[0], p.shape[1] // 8
    width, h = bm // parts, bm // 2

    def theirs(order_ref, *refs):
        for c in range(parts):
            refs[-1][c * width:(c + 1) * width, :] = dot(refs[c][...], refs[parts][...], TN).astype(BF16)

    def mine(order_ref, *refs):
        outs, step = refs[parts + 2:], pl.program_id(0)
        for c in range(parts):
            r = slice(c * width, (c + 1) * width)
            t = dot(refs[c][...], refs[parts][...], TN)
            refs[parts + 1][r, :] = (t + refs[parts + 1][r, :].astype(F32)).astype(BF16)
        for i in range(4):
            @pl.when(step == i)
            def _():
                put(outs, 2 * i, refs[parts + 1][:h, :])
                put(outs, 2 * i + 1, refs[parts + 1][h:, :])

    ins = [pl.BlockSpec((T, width), functools.partial(lambda c, i, o: (0, c * 8 + o[i]), c)) for c in range(parts)]
    ins.append(pl.BlockSpec((T, D), lambda i, o: (0, 0), pipeline_mode=ONE))
    args = [order, *[p] * parts, d]
    block = pl.BlockSpec((bm, D), lambda i, o: (i, 0))
    outs = [(block, shape((n * bm, D), BF16))]
    if got is not None:
        ins.append(block)
        args.append(got)
        outs = [(pl.BlockSpec(s, functools.partial(lambda k, i, o: (0,) * k, len(s))), shape(s, BF16)) for s in pieces(n * bm, D)]
    return call(
        theirs if got is None else mine, (n,), ins, outs, 2 * n * bm * T * D, T * n * bm * 2, prefetch=1, sums=sums
    )(*args)


def sent(t, pairs):
    return lax.ppermute(t, "dp", pairs)


def gateup(a, wg, wu, gather, bn=256, bm=512):
    T, D = a.shape
    N = wg.shape[1]

    def body(a_ref, wg_ref, wu_ref, p_ref, u_ref, g_ref):
        for i in range(T // bm):
            r = slice(i * bm, (i + 1) * bm)
            gate = dot(a_ref[r, :], wg_ref[...], NN)
            up = dot(a_ref[r, :], wu_ref[...], NN)
            s = jax.nn.sigmoid(gate)
            silu = gate * s
            p_ref[r, :] = (silu * up).astype(BF16)
            u_ref[r, :] = silu
            g_ref[r, :] = up * (0.5 * (s + silu * (1 - s)))

    col = lambda j: (0, j)
    w, o = pl.BlockSpec((D, bn), col), pl.BlockSpec((T, bn), col)
    return call(
        body, (N // bn,), [pl.BlockSpec((T, D), lambda j: (0, 0), pipeline_mode=ONE), w, w],
        [(o, shape((T, N), BF16)), (o, shape((T, N), F32)), (o, shape((T, N), F32))], 4 * T * D * N, T * N * 10, gather=gather,
    )(a, wg, wu)


def loaded(sources, targets, sems):
    copies = [pltpu.make_async_copy(s, t, sems.at[i]) for i, (s, t) in enumerate(zip(sources, targets))]
    for c in copies:
        c.start()
    return lambda i: copies[i].wait()


def dproduct(dy, wd, by_u, by_g, start, steps, kept, sums=(), bm=256, bn=1024):
    T, D = dy.shape
    N = wd.shape[0]
    n = N // bn

    def body(d_ref, w_hbm, u_ref, g_ref, du_ref, dg_ref, w_ref, sems):
        def all_of(wait):
            for i in range(n):
                wait(i)
                r = slice(i * bn, (i + 1) * bn)
                dp = dot(d_ref[...], w_ref[r, :], NT).astype(BF16).astype(F32)
                du_ref[:, r] = (dp * u_ref[:, r]).astype(BF16)
                dg_ref[:, r] = (dp * g_ref[:, r] * 2.0).astype(BF16)

        @pl.when(pl.program_id(0) == 0)
        def _():
            cuts = [pl.ds(i * bn, bn) for i in range(n)]
            all_of(loaded([w_hbm.at[c] for c in cuts], [w_ref.at[c] for c in cuts], sems))

        @pl.when(pl.program_id(0) != 0)
        def _():
            all_of(lambda i: None)

    row = lambda j: (start + j, 0)
    o = pl.BlockSpec((bm, N), row)
    return call(
        body, (steps,), [pl.BlockSpec((bm, D), row), pl.BlockSpec(memory_space=pl.ANY), o, o],
        [(o, shape((T, N), BF16)), (o, shape((T, N), BF16))], 2 * steps * bm * D * N, steps * bm * N * 12, kept=kept, sums=sums,
        scratch=[pltpu.VMEM((N, D), BF16), pltpu.SemaphoreType.DMA((n,))],
    )(dy, wd, by_u, by_g)


def both(a, dy, wg, wu, wd, start, gather, kept, bn=256, bm=256):
    T, D = a.shape
    N = wg.shape[1]

    def body(a_ref, d_ref, wg_ref, wu_ref, wd_ref, p_ref, du_ref, dg_ref):
        for i in range(T // bm):
            r = slice(i * bm, (i + 1) * bm)
            gate = dot(a_ref[r, :], wg_ref[...], NN)
            up = dot(a_ref[r, :], wu_ref[...], NN)
            dp = dot(d_ref[r, :], wd_ref[...], NT).astype(BF16).astype(F32)
            s = jax.nn.sigmoid(gate)
            silu = gate * s
            p_ref[r, :] = (silu * up).astype(BF16)
            du_ref[r, :] = (dp * silu).astype(BF16)
            dg_ref[r, :] = (dp * up * (s + silu * (1 - s))).astype(BF16)

    col = lambda j: (0, j)
    full = pl.BlockSpec((T, D), lambda j: (0, 0), pipeline_mode=ONE)
    w, o = pl.BlockSpec((D, bn), col), pl.BlockSpec((T, bn), lambda j: (0, start // bn + j))
    return call(
        body, (N // bn,), [full, full, w, w, pl.BlockSpec((bn, D), lambda j: (start // bn + j, 0))],
        [(o, shape((T, wd.shape[0]), BF16))] * 3, 6 * T * D * N, T * N * 6, gather=gather, kept=kept,
    )(a, dy, wg, wu, wd)


def dnormed(dg, wgs, du, wus, h, g, start, steps, kept, sums=(), bm=256):
    n = len(wgs)
    T, K = dg.shape
    D = wgs[0].shape[0]
    cuts, at = [], 0
    for p, w in enumerate(wgs):
        each = next(c for c in (1280, 1024, 768) if w.shape[1] % c == 0)
        for i in range(w.shape[1] // each):
            cuts.append((p, i * each, at + i * each, each))
        at += w.shape[1]

    def body(dg_ref, du_ref, *refs):
        h_ref, g_ref, o_ref, wg_ref, wu_ref, da_ref, sems = refs[2 * n:]

        @pl.when(pl.program_id(0) == 0)
        def _():
            sources = [refs[m * n + p].at[:, pl.ds(c, w)] for m in range(2) for p, c, _, w in cuts]
            targets = [r.at[:, pl.ds(c, w)] for r in (wg_ref, wu_ref) for _, _, c, w in cuts]
            wait = loaded(sources, targets, sems)
            sums = []
            for m, (d_ref, w_ref) in enumerate(((dg_ref, wg_ref), (du_ref, wu_ref))):
                total = None
                for i, (_, _, c, w) in enumerate(cuts):
                    wait(m * len(cuts) + i)
                    t = dot(d_ref[:, c:c + w], w_ref[:, c:c + w], NT)
                    total = t if total is None else total + t
                sums.append(total.astype(BF16))
            da_ref[...] = sums[0] + sums[1]

        @pl.when(pl.program_id(0) != 0)
        def _():
            da_ref[...] = dot(dg_ref[...], wg_ref[...], NT).astype(BF16) + dot(du_ref[...], wu_ref[...], NT).astype(BF16)

        da, wide = da_ref[...].astype(F32), h_ref[...].astype(F32)
        scale = lax.rsqrt(jnp.mean(wide**2, -1, keepdims=True) + 1e-6)
        inner = jnp.mean(da * wide, -1, keepdims=True)
        o_ref[...] = g_ref[...] + (da * scale - wide * (scale * scale * scale * inner)).astype(BF16)

    row = lambda i: (start + i, 0)
    d, o = pl.BlockSpec((bm, K), row), pl.BlockSpec((bm, D), row)
    return call(
        body, (steps,), [d, d, *[pl.BlockSpec(memory_space=pl.ANY)] * (2 * n), o, o], [(o, shape((T, D), BF16))],
        4 * steps * bm * K * D, steps * bm * K * 4, kept=kept, sums=sums,
        scratch=[pltpu.VMEM((D, K), BF16)] * 2 + [pltpu.VMEM((bm, D), BF16), pltpu.SemaphoreType.DMA((2 * len(cuts),))],
    )(dg, du, *wgs, *wus, h, g)


def down(p, w, h, gather, bm=256, bk=1024):
    T, K = p.shape
    D = w.shape[1]
    n = K // bk

    def body(p_ref, w_hbm, h_ref, o_ref, a_ref, t_ref, w_ref, sems):
        @pl.when(pl.program_id(0) == 0)
        def _():
            cuts = [pl.ds(i * bk, bk) for i in range(n)]
            wait = loaded([w_hbm.at[c] for c in cuts], [w_ref.at[c] for c in cuts], sems)
            total = None
            for i in range(n):
                wait(i)
                t = dot(p_ref[:, i * bk:(i + 1) * bk], w_ref[i * bk:(i + 1) * bk, :], NN)
                total = t if total is None else total + t
            o_ref[...] = h_ref[...] + total.astype(BF16)

        @pl.when(pl.program_id(0) != 0)
        def _():
            o_ref[...] = h_ref[...] + dot(p_ref[...], w_ref[...], NN).astype(BF16)

        norm(o_ref, a_ref, t_ref)

    row = lambda i: (i, 0)
    o = pl.BlockSpec((bm, D), row)
    s = shape((T, D), BF16)
    return call(
        body, (T // bm,), [pl.BlockSpec((bm, K), row), pl.BlockSpec(memory_space=pl.ANY), o],
        [(o, s), (o, s), (pl.BlockSpec((D, bm), lambda i: (0, i)), shape((D, T), BF16))], 2 * T * K * D, T * K * 2, gather=gather,
        scratch=[pltpu.VMEM((K, D), BF16), pltpu.SemaphoreType.DMA((n,))],
    )(p, w, h)


def norm(h_ref, o_ref, t_ref):
    wide = h_ref[...].astype(F32)
    scale = lax.rsqrt(jnp.mean(wide**2, -1, keepdims=True) + 1e-6)
    o_ref[...] = (wide * scale).astype(BF16)
    b = h_ref.shape[1] // 8
    me, nxt, prv, _ = place()
    opp = 6 - me + 2 * (me % 2)
    for i, d in enumerate((opp, prv, nxt, me)):
        for j, block in ((i, d + 1 - 2 * (d % 2)), (i + 4, d)):
            t_ref[j * b:(j + 1) * b, :] = o_ref[:, pl.ds(pl.multiple_of(block * b, b), b)].T


def normed(h, gather, bm=256):
    T, D = h.shape
    o = pl.BlockSpec((bm, D), lambda i: (i, 0))
    return call(
        norm, (T // bm,), [o], [(o, shape((T, D), BF16)), (pl.BlockSpec((D, bm), lambda i: (0, i)), shape((D, T), BF16))],
        T * D * 8, T * D * 6, gather=gather,
    )(h)


def after(t, *before):
    return lax.optimization_barrier((t, *before))[0]


def started(s):
    to_right, to_left, ra, lb, top, low = s
    return sent(to_right, RIGHT), sent(to_left, LEFT), ra, lb, top, low


def joins(s):
    from_left, from_right, ra, lb, _, _ = s
    return [(ra, (from_left, 0)), (lb, (from_right, 0))]


def on(s, to_right, to_left):
    from_left, from_right, _, _, top, low = s
    near_l, near_r = sent(to_right, RIGHT), sent(to_left, LEFT)
    return [(top, near_l, (from_right, 1)), (low, (from_left, 1), near_r)]


def ended(sums):
    h, c = sums[0][0].shape
    terms = [plane_of(t) for group in sums for t in group]

    def body(*refs):
        at = 0
        for i, group in enumerate(sums):
            total = refs[at][...].astype(F32)
            for t in refs[at + 1:at + len(group)]:
                total = total + t[...].astype(F32)
            refs[-1][i // 2, i % 2 * h:(i % 2 + 1) * h, :] = total.astype(BF16)
            at += len(group)

    col = c // 4
    ins = [
        pl.BlockSpec((h, col), lambda j: (0, j)) if p is None else pl.BlockSpec((None, h, col), functools.partial(lambda p, j: (p, 0, j), p))
        for _, p in terms
    ]
    return call(
        body, (4,), ins,
        [(pl.BlockSpec((len(sums) // 2, 2 * h, col), lambda j: (0, 0, j)), shape((len(sums) // 2, 2 * h, c), BF16))], h * c * 8, h * c * 24,
    )(*(t for t, _ in terms))


def summed(sums):
    return call(lambda *refs: None, (4,), [], [], 1000000, 1000000, sums=sums)()


PARTS = (2560, 2048, 1536)


def solution(mesh):
    def body(x, dy, wg, wu, wd):
        order = jnp.asarray(ORDER, jnp.int32)[lax.axis_index("dp")]
        theirs, mine = order[:4], order[4:]
        h0, dy = x[0], dy[0]
        n, FF = wg.shape[1], wg.shape[2]
        own = FF // 8
        offsets = [sum(PARTS[:c]) for c in range(len(PARTS))]
        first, second = lambda r: r.at[0], lambda r: r.at[1]
        cols = lambda c: lambda r: r.at[1, :, pl.ds(offsets[c], PARTS[c])]
        gu = lambda c: [(w, cols(c), (n, PARTS[c])) for w in (wg, wu)]
        a0, at0, wg0, wu0 = normed(h0, Gather(0, [(wg, first, (n, None)), (wu, first, (n, None))], [(7, 8), (7, 8)]))
        act0, u0, g0, wd0, *w1 = gateup(a0, wg0, wu0, Gather(1, [(wd, first, (own, None)), *gu(0)], [(14, 24), (20, 24), (23, 24)]))
        h1, a1, at1, wd1 = down(act0, wd0, h0, Gather(2, [(wd, second, (own, None))], [(7, 8)]))
        act1, du, dg, *w2 = both(a1, dy, *w1, wd1, offsets[0], Gather(3, gu(1), [(3, 7), (6, 8)]), ())
        act1, du, dg, *w3 = both(a1, dy, *w2, wd1, offsets[1], Gather(4, gu(2), [(3, 5), (5, 7)]), (act1, du, dg))
        act1, du, dg = both(a1, dy, *w3, wd1, offsets[2], None, (act1, du, dg))
        wgs, wus = [w1[0], w2[0], w3[0]], [w1[1], w2[1], w3[1]]

        pd = by_blocks(theirs, act1, dy)
        xd = sent(pd, ACROSS)
        pg = by_rows(at1, after(dg, pd), 0)
        xg = sent(pg, ACROSS)
        sd = by_blocks(mine, act1, after(dy, pg), xd)
        rd = started(sd)
        pu = by_rows(at1, after(du, *sd), 0)
        xu = sent(pu, ACROSS)
        sg = by_rows(at1, after(dg, pu), 1, xg)
        rg = started(sg)
        *su, jr, jl = by_rows(at1, after(du, *sg), 1, xu, sums=joins(rd))
        ru = started(su)
        ed = on(rd, jr, jl)
        d1 = dnormed(after(dg, *su), wgs, du, wus, h1, dy, 0, 8, ())
        pd, gr, gl, ur, ul, *dwd1 = by_blocks(theirs, act0, d1, sums=[*joins(rg), *joins(ru), *ed])
        xd = sent(pd, ACROSS)
        eg, eu = on(rg, gr, gl), on(ru, ur, ul)

        du, dg = dproduct(after(d1, pd), wd0, u0, g0, 0, 4, ())
        *sd, gt, gb, ut, ub = by_blocks(mine, act0, after(d1, dg), xd, sums=[*eg, *eu])
        rd = started(sd)
        du, dg = dproduct(after(d1, *sd), wd0, u0, g0, 4, 4, (du, dg))
        pg = by_rows(at0, dg, 0)
        xg = sent(pg, ACROSS)
        pu, jr, jl = by_rows(at0, after(du, pg), 0, sums=joins(rd))
        xu = sent(pu, ACROSS)
        ed = on(rd, jr, jl)
        sg = by_rows(at0, after(dg, pu), 1, xg)
        rg = started(sg)
        *su, dt, db = by_rows(at0, after(du, *sg), 1, xu, sums=ed)
        ru = started(su)
        part = dnormed(after(dg, *su), [wg0], du, [wu0], h0, d1, 0, 5, ())
        _, rg, ru = lax.optimization_barrier((part, rg, ru))
        sums = summed([*joins(rg), *joins(ru)])
        g2, u2 = sums[:2], sums[2:]
        eg, eu = on(rg, *g2), on(ru, *u2)
        d0 = dnormed(after(dg, part, *g2, *u2), [wg0], du, [wu0], h0, d1, 5, 3, (part,))
        dwd = jnp.stack([jnp.concatenate([dt, db]), jnp.concatenate(dwd1)])
        dwg, dwu = ended([*eg, (gt,), (gb,)]), ended([*eu, (ut,), (ub,)])
        return d0[None], dwg, dwu, dwd

    data, rows = P(("rep", "dp"), None, None), P(None, "dp", None)
    out = P("rep", "dp", None)
    return jax.shard_map(body, mesh=mesh, in_specs=(data, data, rows, rows, rows), out_specs=(data, out, out, out), check_vma=False)
```
